32 devices in a mesh: dop: 2 (over core), tm: 16 (over z, y, x).
Axes of the slice: x: 2, y: 2, z: 4, core: 2. Of those that a mesh axis runs over, the one named last changes fastest.
Arguments:
- surveillance: bfloat16 [2, 16, 8192], P(None, 'tm', 'dop'), may hold values from -6 to 6
- reference_signal: bfloat16 [2, 16, 8192], P(None, 'tm', 'dop'), may hold values from -6 to 6
Outputs:
- ambiguity: float32 [2048, 2, 512], P('tm', None, 'dop')
The draws below stay inside these ranges and needn't reach their ends.
All inputs are finite; a program needn't handle non-finite values.
Results may differ from the reference program's by a relative error of at most 0.0029.
Values may be sent and summed in bfloat16 or wider, within the bound.
No kernel may reach another device: no remote copies, remote signals or barrier semaphores. Data moves between devices by JAX's collectives and lax.ppermute only.
A program may use at most 128 MiB of HBM per device.

```python
import math
import jax
import jax.numpy as jnp
from jax import lax

F = 512
LAGS = 2048
BLOCK = 8192
BLOCKS = 16
TIME = 131072


def levels(own_key, extent, split, least, high):
    loudness = 1.0
    for axis_at, shards_of in split:
        heights = jax.random.uniform(jax.random.fold_in(jax.random.fold_in(own_key, 6), axis_at), (shards_of,), jnp.float32, least / len(split), high / len(split))
        loudness = loudness * jnp.repeat(jnp.exp(heights), extent[axis_at] // shards_of).reshape((-1,) + (1,) * (len(extent) - 1 - axis_at))
    return loudness


def scatter_about(rng, extent, spread, limit, split=(), held_as=jnp.bfloat16):
    entries = spread * jax.random.normal(rng, extent, jnp.float32)
    if split:
        entries = entries * levels(rng, extent, split, -0.22, 0.18)
    return jnp.clip(entries, -limit, limit).astype(held_as)


def setup_inputs(seed: int = 0) -> dict:
    splits = jax.random.split(jax.random.key(seed), 3)
    return {
        "surveillance": scatter_about(splits[0], (2, BLOCKS, BLOCK), 1.0, 6.0, ((1, 16), (2, 2))),
        "reference_signal": scatter_about(splits[1], (2, BLOCKS, BLOCK), 1.0, 6.0, ((1, 16), (2, 2))),
    }


def toeplitz_rows(segment, height, breadth):
    length = height + breadth - 1
    repeated = jnp.tile(segment, (1, height + 1))[:, :height * (length + 1)]
    return repeated.reshape(2, height, length + 1)[:, :, :breadth]

def mix_rows(samples, sample_index, doppler, window):
    phase_step = jnp.mod(doppler[:, None] * sample_index[None, :], window)
    phase_angle = phase_step.astype(jnp.float32) * (2.0 * math.pi / window)
    cosine = jnp.cos(phase_angle)
    sine_part = jnp.sin(phase_angle)
    real_in = samples[0].astype(jnp.float32)[None, :]
    imag_in = samples[1].astype(jnp.float32)[None, :]
    mixed_real = (real_in * cosine + imag_in * sine_part).astype(jnp.bfloat16)
    mixed_imag = (imag_in * cosine - real_in * sine_part).astype(jnp.bfloat16)
    upper_half = jnp.concatenate([mixed_real, mixed_imag], 1)
    lower_half = jnp.concatenate([mixed_imag, -mixed_real], 1)
    return jnp.concatenate([upper_half, lower_half], 0)

def lag_product(toeplitz, mixed):
    height = toeplitz.shape[1]
    stacked = toeplitz.reshape(2 * height, toeplitz.shape[2])
    return lax.dot_general(stacked, mixed, (((0,), (1,)), ((), ())), preferred_element_type=jnp.float32)

def reference(surveillance, reference_signal):
    signal = surveillance.reshape(2, TIME)
    reference_flat = reference_signal.reshape(2, TIME)
    extended = jnp.concatenate([jnp.zeros((2, LAGS - 1), jnp.bfloat16), reference_flat], 1)
    height = min(512, TIME)
    doppler = jnp.arange(F, dtype=jnp.int32) - F // 2

    def one_step(running, turn_no):
        offset = turn_no * height
        segment = lax.dynamic_slice_in_dim(extended, offset, height + LAGS - 1, 1)[:, ::-1]
        toeplitz = toeplitz_rows(segment, height, LAGS)
        samples = lax.dynamic_slice_in_dim(signal, offset, height, 1)[:, ::-1]
        sample_index = offset + height - 1 - jnp.arange(height, dtype=jnp.int32)
        return (running + lag_product(toeplitz, mix_rows(samples, sample_index, doppler, TIME)), None)
    running, unused = lax.scan(one_step, jnp.zeros((LAGS, 2 * F), jnp.float32), jnp.arange(TIME // height, dtype=jnp.int32))
    return running.reshape(LAGS, 2, F) * (1.0 / math.sqrt(TIME))
```

```python
import functools
import math

import jax
import jax.numpy as jnp
import numpy as np
from jax import lax
from jax.experimental import pallas as pl
from jax.experimental.pallas import tpu as pltpu
from jax.sharding import PartitionSpec as P

F = 512
LAGS = 2048
LANES = 128


def unit(turns_num, turns_den):
    angle = 2.0 * np.pi * np.mod(turns_num, turns_den) / turns_den
    return np.cos(angle), np.sin(angle)


def body(pos_ref, g_ref, d_ref, mix_ref, kap_ref, tw_ref, place_ref, out_ref, s_ref, rp_ref, rx_ref, acc_ref,
         *, chunks, rows, groups, pad, lags, half, per_step):
    step = pl.program_id(0)

    @pl.when(step == 0)
    def _():
        acc_ref[...] = jnp.zeros_like(acc_ref)
        rp_ref[0:pad] = jnp.zeros((pad, 2, rows, LANES), jnp.float32)

        def first(c, _):
            sr = g_ref[c, 0].astype(jnp.float32)
            si = g_ref[c, 1].astype(jnp.float32)
            tr, ti = mix_ref[0], mix_ref[1]
            kr, ki = kap_ref[0, c], kap_ref[1, c]
            mr = tr * kr - ti * ki
            mi = tr * ki + ti * kr
            s_ref[c, 0] = sr * mr - si * mi
            s_ref[c, 1] = sr * mi + si * mr
            rp_ref[pad + c, 0] = g_ref[c, 2].astype(jnp.float32)
            rp_ref[pad + c, 1] = g_ref[c, 3].astype(jnp.float32)
            return 0

        lax.fori_loop(0, chunks, first, 0)
        lane = lax.broadcasted_iota(jnp.int32, (rows, LANES), 1)
        base = pos_ref[0]

        for grp in range(groups):
            shift = base + grp
            whole = shift // LANES
            part = shift - whole * LANES

            def second(c, _):
                at = c + pad - whole
                for ri in range(2):
                    cur = pltpu.roll(rp_ref[at, ri], part, 1)
                    prev = pltpu.roll(rp_ref[at - 1, ri], part, 1)
                    rx_ref[c, ri, grp * rows : (grp + 1) * rows, :] = jnp.where(lane >= part, cur, prev)
                return 0

            lax.fori_loop(0, chunks, second, 0)

    total = None
    for pair in range(chunks // 2):
        real_rows = []
        for inner in range(per_step):
            a = step * per_step + inner
            start = rows - 1 - a
            yr, yi = [], []
            for c in (2 * pair, 2 * pair + 1):
                rr = rx_ref[c, 0, pl.ds(start, lags), :]
                ri = rx_ref[c, 1, pl.ds(start, lags), :]
                sr = s_ref[c, 0, pl.ds(a, 1), :]
                si = s_ref[c, 1, pl.ds(a, 1), :]
                yr.append((sr * rr + si * ri).astype(jnp.bfloat16))
                yi.append((si * rr - sr * ri).astype(jnp.bfloat16))
            real_rows.append(jnp.concatenate(yr, 1))
            real_rows.append(jnp.concatenate(yi, 1))
        lhs = jnp.concatenate(real_rows, 0)
        term = jnp.dot(lhs, d_ref[pair], preferred_element_type=jnp.float32)
        total = term if total is None else total + term

    sums = [acc_ref[i] for i in range(4)]
    for inner in range(per_step):
        a = step * per_step + inner
        cosine = tw_ref[0, pl.ds(a, 1), :]
        sine = tw_ref[1, pl.ds(a, 1), :]
        for ri in range(2):
            z = total[(2 * inner + ri) * lags : (2 * inner + ri + 1) * lags]
            c, d = z[:, :half], z[:, half:]
            sums[2 * ri] = sums[2 * ri] + (c * cosine - d * sine)
            sums[2 * ri + 1] = sums[2 * ri + 1] + (d * cosine + c * sine)
    for i in range(4):
        acc_ref[i] = sums[i]

    @pl.when(step == pl.num_programs(0) - 1)
    def _():
        cr, dr, ci, di = sums
        put = functools.partial(
            jnp.dot, preferred_element_type=jnp.float32, precision=lax.Precision.HIGHEST
        )
        up, down = place_ref[0], place_ref[1]
        out_ref[:, 0, :] = put(cr + di, up) + put(cr - di, down)
        out_ref[:, 1, :] = put(ci - dr, up) + put(ci + dr, down)


def gather(value, tm, dop):
    return lax.all_gather(value, ("tm", "dop"), axis=0, tiled=False)


def on_device(surveillance, reference_signal):
    pieces = surveillance.shape[2]
    assert surveillance.shape[1] == 1
    tm, dop = lax.axis_size("tm"), lax.axis_size("dop")
    chunks = tm * dop
    window = pieces * chunks
    rows = pieces // LANES
    lags = LAGS // tm
    bins = F // dop
    half = max(bins // 2, LANES)
    groups = 1 + -(-(lags - 1) // rows)
    longest = (LAGS - lags) // rows + groups - 1
    pad = longest // LANES + 1
    per_step = min(4, rows)

    local = jnp.concatenate([surveillance, reference_signal], 0).reshape(4, LANES, rows).transpose(0, 2, 1)
    local = jnp.concatenate([local[:2], local[2:, ::-1]], 0)
    gathered = gather(local, tm, dop)

    half_bins = 2 * np.arange(bins // 2) + 1
    b = np.arange(chunks * LANES, dtype=np.int64)
    spread = np.zeros((chunks * LANES, 2, half))
    cosine, sine = unit(half_bins[None, :] * b[:, None], 2 * chunks * LANES)
    spread[:, 0, : bins // 2], spread[:, 1, : bins // 2] = cosine, sine
    spread = jnp.asarray(spread.reshape(chunks // 2, 2 * LANES, 2 * half), jnp.bfloat16)
    twiddle = np.zeros((2, rows, half), np.float32)
    cosine, sine = unit(half_bins[None, :] * np.arange(rows)[:, None], 2 * window)
    twiddle[0, :, : bins // 2], twiddle[1, :, : bins // 2] = cosine, sine
    twiddle = jnp.asarray(twiddle / math.sqrt(window))
    place = np.zeros((2, half, bins), np.float32)
    for j in range(bins // 2):
        place[0, j, bins // 2 + j] = 1.0
        place[1, j, bins // 2 - 1 - j] = 1.0
    centre = -F + 2 * bins * np.arange(dop) + bins - 1
    inside = np.arange(rows)[:, None] + rows * np.arange(LANES)[None, :]
    cosine, sine = unit(centre[:, None, None] * inside[None], 2 * window)
    mix = np.stack([cosine, -sine], 1).astype(np.float32)
    cosine, sine = unit(centre[:, None] * np.arange(chunks)[None, :], 2 * chunks)
    kappa = np.broadcast_to(np.stack([cosine, -sine], 1)[:, :, :, None, None], (dop, 2, chunks, 1, LANES))
    mine = lax.axis_index("dop")
    mix = lax.dynamic_index_in_dim(jnp.asarray(mix), mine, 0, keepdims=False)
    kappa = lax.dynamic_index_in_dim(jnp.asarray(kappa, jnp.float32), mine, 0, keepdims=False)
    first_shift = (lax.axis_index("tm") * (lags // rows)).astype(jnp.int32).reshape(1)

    vmem = pl.BlockSpec(memory_space=pltpu.VMEM)
    return pl.pallas_call(
        functools.partial(body, chunks=chunks, rows=rows, groups=groups, pad=pad, lags=lags, half=half,
                          per_step=per_step),
        out_shape=jax.ShapeDtypeStruct((lags, 2, bins), jnp.float32),
        grid=(rows // per_step,),
        in_specs=[pl.BlockSpec(memory_space=pltpu.SMEM)] + [vmem] * 6,
        out_specs=vmem,
        scratch_shapes=[
            pltpu.VMEM((chunks, 2, rows, LANES), jnp.float32),
            pltpu.VMEM((pad + chunks, 2, rows, LANES), jnp.float32),
            pltpu.VMEM((chunks, 2, groups * rows, LANES), jnp.float32),
            pltpu.VMEM((4, lags, half), jnp.float32),
        ],
        compiler_params=pltpu.CompilerParams(
            dimension_semantics=("arbitrary",), vmem_limit_bytes=60 * 2**20
        ),
    )(first_shift, gathered, spread, mix, kappa, twiddle, jnp.asarray(place))


def solution(mesh):
    return jax.shard_map(
        on_device,
        mesh=mesh,
        in_specs=(P(None, "tm", "dop"), P(None, "tm", "dop")),
        out_specs=P("tm", None, "dop"),
        check_vma=False,
    )
```

```python
import functools
import math

import jax
import jax.numpy as jnp
import numpy as np
from jax import lax
from jax.experimental import pallas as pl
from jax.experimental.pallas import tpu as pltpu
from jax.sharding import PartitionSpec as P

F = 512
LAGS = 2048
LANES = 128


def unit(turns_num, turns_den):
    angle = 2.0 * np.pi * np.mod(turns_num, turns_den) / turns_den
    return np.cos(angle), np.sin(angle)


def body(pos_ref, g_ref, d_ref, mix_ref, kap_ref, tw_ref, place_ref, out_ref, s_ref, rp_ref, rx_ref, acc_ref,
         *, chunks, rows, groups, pad, lags, half, per_step):
    step = pl.program_id(0)

    @pl.when(step == 0)
    def _():
        acc_ref[...] = jnp.zeros_like(acc_ref)
        rp_ref[0:pad] = jnp.zeros((pad, 2, rows, LANES), jnp.float32)

        def first(c, _):
            sr = g_ref[c, 0].astype(jnp.float32)
            si = g_ref[c, 1].astype(jnp.float32)
            tr, ti = mix_ref[0], mix_ref[1]
            kr, ki = kap_ref[0, c], kap_ref[1, c]
            mr = tr * kr - ti * ki
            mi = tr * ki + ti * kr
            s_ref[c, 0] = sr * mr - si * mi
            s_ref[c, 1] = sr * mi + si * mr
            rp_ref[pad + c, 0] = g_ref[c, 2].astype(jnp.float32)
            rp_ref[pad + c, 1] = g_ref[c, 3].astype(jnp.float32)
            return 0

        lax.fori_loop(0, chunks, first, 0)
        lane = lax.broadcasted_iota(jnp.int32, (rows, LANES), 1)
        base = pos_ref[0]

        for grp in range(groups):
            shift = base + grp
            whole = shift // LANES
            part = shift - whole * LANES

            def second(c, _):
                at = c + pad - whole
                for ri in range(2):
                    cur = pltpu.roll(rp_ref[at, ri], part, 1)
                    prev = pltpu.roll(rp_ref[at - 1, ri], part, 1)
                    rx_ref[c, ri, grp * rows : (grp + 1) * rows, :] = jnp.where(lane >= part, cur, prev)
                return 0

            lax.fori_loop(0, chunks, second, 0)

    total = None
    for pair in range(chunks // 2):
        real_rows = []
        for inner in range(per_step):
            a = step * per_step + inner
            start = rows - 1 - a
            yr, yi = [], []
            for c in (2 * pair, 2 * pair + 1):
                rr = rx_ref[c, 0, pl.ds(start, lags), :]
                ri = rx_ref[c, 1, pl.ds(start, lags), :]
                sr = s_ref[c, 0, pl.ds(a, 1), :]
                si = s_ref[c, 1, pl.ds(a, 1), :]
                yr.append((sr * rr + si * ri).astype(jnp.bfloat16))
                yi.append((si * rr - sr * ri).astype(jnp.bfloat16))
            real_rows.append(jnp.concatenate(yr, 1))
            real_rows.append(jnp.concatenate(yi, 1))
        lhs = jnp.concatenate(real_rows, 0)
        term = jnp.dot(lhs, d_ref[pair], preferred_element_type=jnp.float32)
        total = term if total is None else total + term

    sums = [acc_ref[i] for i in range(4)]
    for inner in range(per_step):
        a = step * per_step + inner
        cosine = tw_ref[0, pl.ds(a, 1), :]
        sine = tw_ref[1, pl.ds(a, 1), :]
        for ri in range(2):
            z = total[(2 * inner + ri) * lags : (2 * inner + ri + 1) * lags]
            c, d = z[:, :half], z[:, half:]
            sums[2 * ri] = sums[2 * ri] + (c * cosine - d * sine)
            sums[2 * ri + 1] = sums[2 * ri + 1] + (d * cosine + c * sine)
    for i in range(4):
        acc_ref[i] = sums[i]

    @pl.when(step == pl.num_programs(0) - 1)
    def _():
        cr, dr, ci, di = sums
        put = functools.partial(
            jnp.dot, preferred_element_type=jnp.float32, precision=lax.Precision.HIGHEST
        )
        up, down = place_ref[0], place_ref[1]
        out_ref[:, 0, :] = put(cr + di, up) + put(cr - di, down)
        out_ref[:, 1, :] = put(ci - dr, up) + put(ci + dr, down)


def gather(value, tm, dop):
    copies = jnp.broadcast_to(value[None], (tm * dop,) + value.shape)
    return lax.all_to_all(copies, ("tm", "dop"), 0, 0)


def on_device(surveillance, reference_signal):
    pieces = surveillance.shape[2]
    assert surveillance.shape[1] == 1
    tm, dop = lax.axis_size("tm"), lax.axis_size("dop")
    chunks = tm * dop
    window = pieces * chunks
    rows = pieces // LANES
    lags = LAGS // tm
    bins = F // dop
    half = max(bins // 2, LANES)
    groups = 1 + -(-(lags - 1) // rows)
    longest = (LAGS - lags) // rows + groups - 1
    pad = longest // LANES + 1
    per_step = min(4, rows)

    local = jnp.concatenate([surveillance, reference_signal], 0).reshape(4, LANES, rows).transpose(0, 2, 1)
    local = jnp.concatenate([local[:2], local[2:, ::-1]], 0)
    gathered = gather(local, tm, dop)

    half_bins = 2 * np.arange(bins // 2) + 1
    b = np.arange(chunks * LANES, dtype=np.int64)
    spread = np.zeros((chunks * LANES, 2, half))
    cosine, sine = unit(half_bins[None, :] * b[:, None], 2 * chunks * LANES)
    spread[:, 0, : bins // 2], spread[:, 1, : bins // 2] = cosine, sine
    spread = jnp.asarray(spread.reshape(chunks // 2, 2 * LANES, 2 * half), jnp.bfloat16)
    twiddle = np.zeros((2, rows, half), np.float32)
    cosine, sine = unit(half_bins[None, :] * np.arange(rows)[:, None], 2 * window)
    twiddle[0, :, : bins // 2], twiddle[1, :, : bins // 2] = cosine, sine
    twiddle = jnp.asarray(twiddle / math.sqrt(window))
    place = np.zeros((2, half, bins), np.float32)
    for j in range(bins // 2):
        place[0, j, bins // 2 + j] = 1.0
        place[1, j, bins // 2 - 1 - j] = 1.0
    centre = -F + 2 * bins * np.arange(dop) + bins - 1
    inside = np.arange(rows)[:, None] + rows * np.arange(LANES)[None, :]
    cosine, sine = unit(centre[:, None, None] * inside[None], 2 * window)
    mix = np.stack([cosine, -sine], 1).astype(np.float32)
    cosine, sine = unit(centre[:, None] * np.arange(chunks)[None, :], 2 * chunks)
    kappa = np.broadcast_to(np.stack([cosine, -sine], 1)[:, :, :, None, None], (dop, 2, chunks, 1, LANES))
    mine = lax.axis_index("dop")
    mix = lax.dynamic_index_in_dim(jnp.asarray(mix), mine, 0, keepdims=False)
    kappa = lax.dynamic_index_in_dim(jnp.asarray(kappa, jnp.float32), mine, 0, keepdims=False)
    first_shift = (lax.axis_index("tm") * (lags // rows)).astype(jnp.int32).reshape(1)

    vmem = pl.BlockSpec(memory_space=pltpu.VMEM)
    return pl.pallas_call(
        functools.partial(body, chunks=chunks, rows=rows, groups=groups, pad=pad, lags=lags, half=half,
                          per_step=per_step),
        out_shape=jax.ShapeDtypeStruct((lags, 2, bins), jnp.float32),
        grid=(rows // per_step,),
        in_specs=[pl.BlockSpec(memory_space=pltpu.SMEM)] + [vmem] * 6,
        out_specs=vmem,
        scratch_shapes=[
            pltpu.VMEM((chunks, 2, rows, LANES), jnp.float32),
            pltpu.VMEM((pad + chunks, 2, rows, LANES), jnp.float32),
            pltpu.VMEM((chunks, 2, groups * rows, LANES), jnp.float32),
            pltpu.VMEM((4, lags, half), jnp.float32),
        ],
        compiler_params=pltpu.CompilerParams(
            dimension_semantics=("arbitrary",), vmem_limit_bytes=60 * 2**20
        ),
    )(first_shift, gathered, spread, mix, kappa, twiddle, jnp.asarray(place))


def solution(mesh):
    return jax.shard_map(
        on_device,
        mesh=mesh,
        in_specs=(P(None, "tm", "dop"), P(None, "tm", "dop")),
        out_specs=P("tm", None, "dop"),
        check_vma=False,
    )
```
